32 devices in a mesh: groups: 2 (over y), ctx: 4 (over z), head: 2 (over x), rep: 2 (over core).
Axes of the slice: x: 2, y: 2, z: 4, core: 2. Of those that a mesh axis runs over, the one named last changes fastest.
Arguments:
- queries: bfloat16 [2048, 4096], P(('groups', 'ctx'), ('head', 'rep')), parts along dimension 0, may hold values from -24 to 24
- keys: bfloat16 [2048, 1024], P(('groups', 'ctx'), ('head', 'rep')), parts along dimension 0, may hold values from -6 to 6
- values: bfloat16 [2048, 1024], P(('groups', 'ctx'), ('head', 'rep')), parts along dimension 0, may hold values from -6 to 6
- span_order: int32 [8], replicated, may hold values from 0 to 7, as said below
Outputs:
- attended: bfloat16 [2048, 4096], P(('groups', 'ctx'), ('head', 'rep')), parts along dimension 0
The draws below stay inside these ranges and needn't reach their ends.
There are 2 independent parts, one for each index of `groups`. The reference program is written for one: setup_inputs(seed, part) draws one part's arguments, and reference() takes and returns one part's arrays. A program takes and returns all parts, laid end to end along the dimension named above; an argument that names none is the same for every part. Nothing has to cross between parts.
Inputs may be any that keep to these rules, and one draw needn't show every extreme that they name: `span_order`: A permutation of the spans in which entries 2 d and 2 d + 1 are c and 7 - c for some c.
All inputs are finite; a program needn't handle non-finite values.
Results may differ from the reference program's by a relative error of at most 0.0047.
Values may be sent and summed in bfloat16 or wider, within the bound.
A program may use at most 64 MiB of HBM per device.

```python
import math
import jax
import jax.numpy as jnp
from jax import lax

QUERY_HEADS = 32
KEY_VALUE_HEADS = 8
HEAD_SIZE = 128
SPAN = 128
SPANS = 8
SEQUENCE_TOKENS = 1024


def draw_queries(key, part):
    perturb_random_key = jax.random.fold_in(key, 21)
    scale_key = jax.random.fold_in(key, 22)
    noise = jax.random.truncated_normal(perturb_random_key, -4.0, 4.0, (SEQUENCE_TOKENS, QUERY_HEADS, HEAD_SIZE), jnp.float32)
    row_scale = jnp.exp(jax.random.uniform(scale_key, (SEQUENCE_TOKENS, QUERY_HEADS, 1), jnp.float32, 0.0, math.log(6.0)))
    sampled_values = noise * row_scale
    return sampled_values.reshape(SEQUENCE_TOKENS, QUERY_HEADS * HEAD_SIZE).astype(jnp.bfloat16)


def draw_keys(key, part):
    perturb_random_key = jax.random.fold_in(key, 31)
    sampled_values = jax.random.truncated_normal(perturb_random_key, -6.0, 6.0, (SEQUENCE_TOKENS, KEY_VALUE_HEADS, HEAD_SIZE), jnp.float32)
    return sampled_values.reshape(SEQUENCE_TOKENS, KEY_VALUE_HEADS * HEAD_SIZE).astype(jnp.bfloat16)


def draw_span_order(key, part):
    pair_count = SPANS // 2
    pair_order = jax.random.permutation(jax.random.fold_in(key, 41), pair_count)
    flip_bits = jax.random.randint(jax.random.fold_in(key, 42), (pair_count,), 0, 2)
    first_span = jnp.where(flip_bits == 1, pair_order, SPANS - 1 - pair_order)
    second_span = SPANS - 1 - first_span
    return jnp.stack([first_span, second_span], axis=1).reshape(SPANS).astype(jnp.int32)


def block_levels(key, extent, pieces, low, high):
    factor_of = 1.0
    for axis_at, blocks in pieces:
        steps = jax.random.uniform(jax.random.fold_in(jax.random.fold_in(key, 6), axis_at), (blocks,), jnp.float32, low / len(pieces), high / len(pieces))
        factor_of = factor_of * jnp.repeat(jnp.exp(steps), extent[axis_at] // blocks).reshape((-1,) + (1,) * (len(extent) - 1 - axis_at))
    return factor_of


def bell_draw(stream_key, shape, scale, most, cuts=(), kind=jnp.bfloat16):
    result = jax.random.normal(stream_key, shape, jnp.float32) * scale
    if len(cuts) > 0:
        result = block_levels(stream_key, shape, cuts, -0.22, 0.18) * result
    return jnp.clip(result, min=-most, max=most).astype(kind)


def setup_inputs(seed: int = 0, part: int = 0) -> dict:
    arg_keys = jax.random.split(jax.random.key(seed), 5)
    part_keys = jax.random.split(jax.random.fold_in(arg_keys[4], part), 5)
    queries = draw_queries(jax.random.fold_in(jax.random.fold_in(arg_keys[4], part), 71), part)
    keys = draw_keys(jax.random.fold_in(jax.random.fold_in(arg_keys[4], part), 71), part)
    values = bell_draw(part_keys[2], (SEQUENCE_TOKENS, KEY_VALUE_HEADS * HEAD_SIZE), 1.0, 6.0, ((0, 4), (1, 4)))
    span_order = draw_span_order(jax.random.fold_in(arg_keys[4], 71), part)
    return {"queries": queries, "keys": keys, "values": values, "span_order": span_order}


masked_score = -1e+30

def source_partials(query_block, query_pos, key_block, value_block, key_pos):
    score_scale = 1.0 / math.sqrt(HEAD_SIZE)
    scores = jnp.einsum('rhgd,shd->rhgs', query_block, key_block) * score_scale
    allowed = (key_pos[None, :] <= query_pos[:, None])[:, None, None, :]
    masked = jnp.where(allowed, scores, masked_score)
    row_top = lax.optimization_barrier(jnp.max(masked, axis=-1))
    weights = jnp.where(allowed, jnp.exp(masked - row_top[..., None]), 0.0)
    row_total = lax.optimization_barrier(jnp.sum(weights, axis=-1))
    rounded = lax.optimization_barrier(weights.astype(jnp.bfloat16)).astype(jnp.float32)
    numerator = jnp.einsum('rhgs,shd->rhgd', rounded, value_block)
    partial_value = numerator / jnp.maximum(row_total, 1.0)[..., None]
    partial_value = lax.optimization_barrier(partial_value.astype(jnp.bfloat16)).astype(jnp.float32)
    return (partial_value, row_top, row_total)

def reference(queries, keys, values, span_order):
    row_index = jnp.arange(SEQUENCE_TOKENS, dtype=jnp.int32)
    positions = span_order[row_index // SPAN].astype(jnp.int32) * SPAN + row_index % SPAN
    contributor_list = SPANS // 2
    rows_per_block = 2 * SPAN
    common_values = QUERY_HEADS // KEY_VALUE_HEADS
    query_block_list = queries.astype(jnp.float32).reshape(contributor_list, rows_per_block, KEY_VALUE_HEADS, common_values, HEAD_SIZE)
    key_block_list = keys.astype(jnp.float32).reshape(contributor_list, rows_per_block, KEY_VALUE_HEADS, HEAD_SIZE)
    value_block_list = values.astype(jnp.float32).reshape(contributor_list, rows_per_block, KEY_VALUE_HEADS, HEAD_SIZE)
    position_blocks = positions.reshape(contributor_list, rows_per_block)

    def one_block(operands):
        query_block, query_pos = operands

        def one_source(inputs_now):
            return source_partials(query_block, query_pos, inputs_now[0], inputs_now[1], inputs_now[2])
        partials, row_tops, row_totals = lax.map(one_source, (key_block_list, value_block_list, position_blocks))
        best_top = lax.optimization_barrier(jnp.max(row_tops, axis=0))
        source_weight = row_totals * jnp.exp(row_tops - best_top[None])
        weighted = lax.optimization_barrier(jnp.sum(source_weight[..., None] * partials, axis=0))
        return (weighted / lax.optimization_barrier(jnp.sum(source_weight, axis=0))[..., None]).astype(jnp.bfloat16)
    attended = lax.map(one_block, (query_block_list, position_blocks))
    return attended.reshape(SEQUENCE_TOKENS, QUERY_HEADS * HEAD_SIZE)
```

```python
import functools
import math

import jax
import jax.numpy as jnp
from jax import lax
from jax.experimental import pallas as pl
from jax.experimental.pallas import tpu as pltpu
from jax.sharding import PartitionSpec as P

HEAD_SIZE = 128
MASKED = -1e30
MESH = pl.DeviceIdType.MESH
RIGHT, LEFT = 0, 1
KEY, VALUE = 0, 1


def attend(
    n, order_ref, q_hbm, k_hbm, v_hbm, out_ref,
    q_ref, k_ref, v_ref, p_ref, alpha_ref, top_ref, total_ref, acc_ref,
    load_sem, send_sem, recv_sem,
):
    me = lax.axis_index("ctx")
    rows, q_cols = q_ref.shape
    span = rows // 2
    kv_heads = k_ref.shape[2] // HEAD_SIZE
    group = q_cols // HEAD_SIZE // kv_heads
    exponent_scale = math.log2(math.e) / math.sqrt(HEAD_SIZE)
    buffers = (k_ref, v_ref)

    load_k = pltpu.make_async_copy(k_hbm, k_ref.at[me], load_sem.at[0])
    load_v = pltpu.make_async_copy(v_hbm, v_ref.at[me], load_sem.at[1])
    load_q = pltpu.make_async_copy(q_hbm, q_ref, load_sem.at[2])
    load_k.start()
    load_v.start()
    load_q.start()

    has_right, has_left = me < n - 1, me > 0
    barrier = pltpu.get_barrier_semaphore()

    @pl.when(has_right)
    def _():
        pl.semaphore_signal(barrier, inc=1, device_id={"ctx": me + 1}, device_id_type=MESH)

    @pl.when(has_left)
    def _():
        pl.semaphore_signal(barrier, inc=1, device_id={"ctx": me - 1}, device_id_type=MESH)

    pl.semaphore_wait(barrier, jnp.where(has_right, 1, 0) + jnp.where(has_left, 1, 0))

    def hop(way, kind, step, block, target):
        return pltpu.make_async_remote_copy(
            src_ref=buffers[kind].at[block],
            dst_ref=buffers[kind].at[block],
            send_sem=send_sem.at[way, kind, step],
            recv_sem=recv_sem.at[way, kind, step],
            device_id={"ctx": target},
            device_id_type=MESH,
        )

    def pass_right(kind, step):
        return hop(RIGHT, kind, step, me - step, me + 1)

    def pass_left(kind, step):
        return hop(LEFT, kind, step, me + step, me - 1)

    def arrive(kind, step):
        @pl.when(me - step >= 0)
        def _():
            hop(RIGHT, kind, step - 1, me - step, jnp.minimum(me + 1, n - 1)).wait_recv()

            @pl.when(has_right)
            def _():
                pass_right(kind, step).start()

        @pl.when(me + step < n)
        def _():
            hop(LEFT, kind, step - 1, me + step, jnp.maximum(me - 1, 0)).wait_recv()

            @pl.when(has_left)
            def _():
                pass_left(kind, step).start()

    for kind, load in ((KEY, load_k), (VALUE, load_v)):
        load.wait()

        @pl.when(has_right)
        def _():
            pass_right(kind, 0).start()

        @pl.when(has_left)
        def _():
            pass_left(kind, 0).start()

    load_q.wait()

    def positions(block, axis):
        index = lax.broadcasted_iota(jnp.int32, (rows, rows), axis)
        first, second = order_ref[2 * block], order_ref[2 * block + 1]
        return index + jnp.where(index < span, first * span, second * span - span)

    def columns(head):
        return pl.ds(head * HEAD_SIZE, HEAD_SIZE)

    def weigh(block, slot, opening):
        bias = jnp.where(positions(block, 1) <= positions(me, 0), 0.0, MASKED)
        for head in range(kv_heads * group):
            scores = lax.dot_general(
                q_ref[:, columns(head)], k_ref[block, :, columns(head // group)],
                (((1,), (1,)), ((), ())), preferred_element_type=jnp.float32,
            ) + bias
            top = jnp.max(scores, axis=1, keepdims=True)
            if not opening:
                old = top_ref[head][:, :1]
                top = jnp.maximum(old, top)
                alpha = jnp.exp2((old - top) * exponent_scale)
                alpha_ref[slot, head] = jnp.broadcast_to(alpha, (rows, HEAD_SIZE))
            weights = jnp.exp2((scores - top) * exponent_scale)
            total = jnp.sum(weights, axis=1, keepdims=True)
            if not opening:
                total = total_ref[head][:, :1] * alpha + total
            top_ref[head] = jnp.broadcast_to(top, (rows, HEAD_SIZE))
            total_ref[head] = jnp.broadcast_to(total, (rows, HEAD_SIZE))
            p_ref[slot, head] = weights.astype(jnp.bfloat16)

    def gather(block, slot, opening):
        for head in range(kv_heads * group):
            part = jnp.dot(
                p_ref[slot, head], v_ref[block, :, columns(head // group)],
                preferred_element_type=jnp.float32,
            )
            if not opening:
                part = acc_ref[head] * alpha_ref[slot, head] + part
            acc_ref[head] = part

    weigh(me, 0, True)
    gather(me, 0, True)

    def turn(step, carry):
        def each(work):
            @pl.when(me - step >= 0)
            def _():
                work(me - step, 0, False)

            @pl.when(me + step < n)
            def _():
                work(me + step, 1, False)

        arrive(KEY, step)
        each(weigh)
        arrive(VALUE, step)
        each(gather)
        return carry

    lax.fori_loop(1, n, turn, 0)

    for head in range(kv_heads * group):
        out_ref[:, columns(head)] = (acc_ref[head] / total_ref[head]).astype(out_ref.dtype)

    def drain(step, carry):
        for kind in (KEY, VALUE):
            @pl.when((me - step >= 0) & has_right)
            def _():
                pass_right(kind, step).wait_send()

            @pl.when((me + step < n) & has_left)
            def _():
                pass_left(kind, step).wait_send()
        return carry

    lax.fori_loop(0, n - 1, drain, 0)


def shards(n, queries, keys, values, span_order):
    rows, q_cols = queries.shape
    heads = q_cols // HEAD_SIZE
    per_head = (heads, rows, HEAD_SIZE)
    return pl.pallas_call(
        functools.partial(attend, n),
        out_shape=jax.ShapeDtypeStruct((rows, q_cols), jnp.bfloat16),
        in_specs=[pl.BlockSpec(memory_space=pltpu.SMEM)] + [pl.BlockSpec(memory_space=pl.ANY)] * 3,
        out_specs=pl.BlockSpec(memory_space=pltpu.VMEM),
        scratch_shapes=[
            pltpu.VMEM((rows, q_cols), jnp.bfloat16),
            pltpu.VMEM((n,) + keys.shape, jnp.bfloat16),
            pltpu.VMEM((n,) + values.shape, jnp.bfloat16),
            pltpu.VMEM((2, heads, rows, rows), jnp.bfloat16),
            pltpu.VMEM((2,) + per_head, jnp.float32),
            pltpu.VMEM(per_head, jnp.float32),
            pltpu.VMEM(per_head, jnp.float32),
            pltpu.VMEM(per_head, jnp.float32),
            pltpu.SemaphoreType.DMA((3,)),
            pltpu.SemaphoreType.DMA((2, 2, n)),
            pltpu.SemaphoreType.DMA((2, 2, n)),
        ],
        compiler_params=pltpu.CompilerParams(collective_id=0, has_side_effects=True),
    )(span_order, queries, keys, values)


def solution(mesh):
    split = P(("groups", "ctx"), ("head", "rep"))
    return jax.shard_map(
        functools.partial(shards, mesh.shape["ctx"]),
        mesh=mesh,
        in_specs=(split, split, split, P()),
        out_specs=split,
        check_vma=False,
    )
```

```python
import functools
import math

import jax
import jax.numpy as jnp
from jax import lax
from jax.experimental import pallas as pl
from jax.experimental.pallas import tpu as pltpu
from jax.sharding import PartitionSpec as P

HEAD_SIZE = 128
MASKED = -1e30
MESH = pl.DeviceIdType.MESH
KEY, VALUE = 0, 1


def attend(
    n, order_hbm, q_hbm, k_hbm, v_hbm, out_ref,
    order_ref, q_ref, k_ref, v_ref, stack_ref, p_ref, top_ref, acc_ref,
    load_sem, send_sem, recv_sem,
):
    me = lax.axis_index("ctx")
    rows, q_cols = q_ref.shape
    span = rows // 2
    kv_heads = k_ref.shape[2] // HEAD_SIZE
    group = q_cols // HEAD_SIZE // kv_heads
    exponent_scale = math.log2(math.e) / math.sqrt(HEAD_SIZE)
    buffers = (k_ref, v_ref)

    load_k = pltpu.make_async_copy(k_hbm, k_ref.at[me], load_sem.at[0])
    load_v = pltpu.make_async_copy(v_hbm, v_ref.at[me], load_sem.at[1])
    load_order = pltpu.make_async_copy(order_hbm, order_ref, load_sem.at[3])
    load_q = pltpu.make_async_copy(q_hbm, q_ref, load_sem.at[2])
    load_k.start()
    load_v.start()
    load_q.start()
    load_order.start()

    major = jnp.where(me < n // 2, -1, 1)

    def inside(index):
        return (index >= 0) & (index < n)

    barrier = pltpu.get_barrier_semaphore()
    for way in (-1, 1):
        @pl.when(inside(me + way))
        def _():
            pl.semaphore_signal(barrier, inc=1, device_id={"ctx": me + way}, device_id_type=MESH)

    pl.semaphore_wait(barrier, jnp.where(me > 0, 1, 0) + jnp.where(me < n - 1, 1, 0))

    def hop(way, kind, step, block):
        lane = (way + 1) // 2
        return pltpu.make_async_remote_copy(
            src_ref=buffers[kind].at[block],
            dst_ref=buffers[kind].at[block],
            send_sem=send_sem.at[lane, kind, step],
            recv_sem=recv_sem.at[lane, kind, step],
            device_id={"ctx": jnp.clip(me + way, 0, n - 1)},
            device_id_type=MESH,
        )

    def arrive(kind, step):
        for way in (major, -major):
            @pl.when(inside(me - way * step))
            def _():
                hop(way, kind, step - 1, me - way * step).wait_recv()

                @pl.when(inside(me + way))
                def _():
                    hop(way, kind, step, me - way * step).start()

    for kind, load in ((KEY, load_k), (VALUE, load_v)):
        load.wait()
        for way in (major, -major):
            @pl.when(inside(me + way))
            def _():
                hop(way, kind, 0, me).start()

    load_q.wait()
    load_order.wait()

    def columns(head):
        return pl.ds(head * HEAD_SIZE, HEAD_SIZE)

    def low_first(block):
        return order_ref[2 * block] < order_ref[2 * block + 1]

    def low_span(block):
        return jnp.minimum(order_ref[2 * block], order_ref[2 * block + 1])

    def low_high(ref, block, head):
        first, second = ref[block, :span, columns(head)], ref[block, span:, columns(head)]
        swap = low_first(block)
        return jnp.where(swap, first, second), jnp.where(swap, second, first)

    def score(head, part, keys):
        queries = stack_ref[head, part] if isinstance(part, int) else part
        return lax.dot_general(
            queries, keys, (((1,), (1,)), ((), ())), preferred_element_type=jnp.float32
        )

    def peak(scores):
        return jnp.max(scores, axis=1, keepdims=True)

    def weights_of(scores, top):
        return jnp.exp2((scores - top) * exponent_scale).astype(jnp.bfloat16)

    def keep(ref, value):
        ref[...] = jnp.broadcast_to(value, (group * span, HEAD_SIZE))

    def with_ones(values):
        return jnp.concatenate([values, jnp.ones_like(values)], axis=1)

    def product(weights, values):
        return jnp.dot(weights, with_ones(values), preferred_element_type=jnp.float32)

    mine_first = low_first(me)
    for head in range(kv_heads):
        for member in range(group):
            column = columns(head * group + member)
            first, second = q_ref[:span, column], q_ref[span:, column]
            stack_ref[head, 0, member * span : (member + 1) * span] = jnp.where(mine_first, first, second)
            stack_ref[head, 1, member * span : (member + 1) * span] = jnp.where(mine_first, second, first)

    tall = (group * span, span)
    row = lax.rem(lax.broadcasted_iota(jnp.int32, tall, 0), span)
    bias = jnp.where(lax.broadcasted_iota(jnp.int32, tall, 1) <= row, 0.0, MASKED)
    for head in range(kv_heads):
        key_low, key_high = low_high(k_ref, me, head)
        value_low, value_high = low_high(v_ref, me, head)
        low = score(head, 0, key_low) + bias
        low_top = peak(low)
        keep(top_ref.at[head, 0], low_top)
        acc_ref[head, 0] = product(weights_of(low, low_top), value_low)
        cross = score(head, 1, key_low)
        high = score(head, 1, key_high) + bias
        high_top = jnp.maximum(peak(cross), peak(high))
        keep(top_ref.at[head, 1], high_top)
        acc_ref[head, 1] = product(weights_of(cross, high_top), value_low) + product(
            weights_of(high, high_top), value_high
        )

    def weigh(block):
        earlier = low_span(block) < low_span(me)
        for head in range(kv_heads):
            key_low, key_high = low_high(k_ref, block, head)
            cross = score(head, 1, key_low)
            other = score(
                head,
                jnp.where(earlier, stack_ref[head, 0], stack_ref[head, 1]),
                jnp.where(earlier, key_low, key_high),
            )
            other_top = peak(other)
            old_low, old_high = top_ref[head, 0][:, :1], top_ref[head, 1][:, :1]
            low_top = jnp.maximum(old_low, jnp.where(earlier, other_top, MASKED))
            high_top = jnp.maximum(
                jnp.maximum(old_high, peak(cross)), jnp.where(earlier, MASKED, other_top)
            )
            keep(top_ref.at[head, 0], low_top)
            keep(top_ref.at[head, 1], high_top)
            acc_ref[head, 0] *= jnp.exp2((old_low - low_top) * exponent_scale)
            acc_ref[head, 1] *= jnp.exp2((old_high - high_top) * exponent_scale)
            p_ref[head, 0] = weights_of(cross, high_top)
            p_ref[head, 1] = weights_of(other, jnp.where(earlier, low_top, high_top))

    def gather(block):
        earlier = low_span(block) < low_span(me)
        for head in range(kv_heads):
            value_low, value_high = low_high(v_ref, block, head)
            cross = product(p_ref[head, 0], value_low)
            other = product(p_ref[head, 1], jnp.where(earlier, value_low, value_high))
            acc_ref[head, 0] += jnp.where(earlier, other, 0.0)
            acc_ref[head, 1] += cross + jnp.where(earlier, 0.0, other)

    def turn(step, carry):
        arrive(KEY, step)

        @pl.when(inside(me - major * step))
        def _():
            weigh(me - major * step)

        arrive(VALUE, step)

        @pl.when(inside(me - major * step))
        def _():
            gather(me - major * step)

        @pl.when(inside(me + major * step))
        def _():
            weigh(me + major * step)
            gather(me + major * step)

        return carry

    lax.fori_loop(1, n, turn, 0)

    for head in range(kv_heads):
        for member in range(group):
            column = columns(head * group + member)
            part = pl.ds(member * span, span)
            low = acc_ref[head, 0, part, :HEAD_SIZE] / acc_ref[head, 0, part, HEAD_SIZE:]
            high = acc_ref[head, 1, part, :HEAD_SIZE] / acc_ref[head, 1, part, HEAD_SIZE:]
            out_ref[:span, column] = jnp.where(mine_first, low, high).astype(out_ref.dtype)
            out_ref[span:, column] = jnp.where(mine_first, high, low).astype(out_ref.dtype)

    def drain(step, carry):
        for kind in (KEY, VALUE):
            for way in (major, -major):
                @pl.when(inside(me - way * step) & inside(me + way))
                def _():
                    hop(way, kind, step, me - way * step).wait_send()
        return carry

    lax.fori_loop(0, n - 1, drain, 0)


def shards(n, queries, keys, values, span_order):
    rows, q_cols = queries.shape
    span = rows // 2
    kv_heads = keys.shape[1] // HEAD_SIZE
    tall = q_cols // HEAD_SIZE // kv_heads * span
    inputs = [pltpu.with_memory_space_constraint(x, pltpu.HBM) for x in (span_order, queries, keys, values)]
    return pl.pallas_call(
        functools.partial(attend, n),
        out_shape=jax.ShapeDtypeStruct((rows, q_cols), jnp.bfloat16),
        in_specs=[pl.BlockSpec(memory_space=pltpu.HBM)] * 4,
        out_specs=pl.BlockSpec(memory_space=pltpu.VMEM),
        scratch_shapes=[
            pltpu.SMEM(span_order.shape, jnp.int32),
            pltpu.VMEM((rows, q_cols), jnp.bfloat16),
            pltpu.VMEM((n,) + keys.shape, jnp.bfloat16),
            pltpu.VMEM((n,) + values.shape, jnp.bfloat16),
            pltpu.VMEM((kv_heads, 2, tall, HEAD_SIZE), jnp.bfloat16),
            pltpu.VMEM((kv_heads, 2, tall, span), jnp.bfloat16),
            pltpu.VMEM((kv_heads, 2, tall, HEAD_SIZE), jnp.float32),
            pltpu.VMEM((kv_heads, 2, tall, 2 * HEAD_SIZE), jnp.float32),
            pltpu.SemaphoreType.DMA((4,)),
            pltpu.SemaphoreType.DMA((2, 2, n)),
            pltpu.SemaphoreType.DMA((2, 2, n)),
        ],
        compiler_params=pltpu.CompilerParams(
            collective_id=0, has_side_effects=True, vmem_limit_bytes=32 * 2**20
        ),
    )(*inputs)


def solution(mesh):
    split = P(("groups", "ctx"), ("head", "rep"))
    return jax.shard_map(
        functools.partial(shards, mesh.shape["ctx"]),
        mesh=mesh,
        in_specs=(split, split, split, P()),
        out_specs=split,
        check_vma=False,
    )
```

```python
import functools
import math

import jax
import jax.numpy as jnp
from jax import lax
from jax.experimental import pallas as pl
from jax.experimental.pallas import tpu as pltpu
from jax.sharding import PartitionSpec as P

HEAD_SIZE = 128
MASKED = -1e30
MESH = pl.DeviceIdType.MESH
KEY, VALUE = 0, 1


def attend(
    n, order_hbm, q_hbm, k_hbm, v_hbm, out_ref,
    order_ref, q_ref, k_ref, v_ref, stack_ref, p_ref, top_ref, acc_ref,
    load_sem, send_sem, recv_sem,
):
    me = lax.axis_index("ctx")
    rows, q_cols = q_ref.shape
    span = rows // 2
    kv_heads = k_ref.shape[1]
    group = q_cols // HEAD_SIZE // kv_heads
    exponent_scale = math.log2(math.e) / math.sqrt(HEAD_SIZE)
    buffers = (k_ref, v_ref)

    def columns(head):
        return pl.ds(head * HEAD_SIZE, HEAD_SIZE)

    pieces = [(kind, head) for kind in (KEY, VALUE) for head in range(kv_heads)]
    loads = [
        pltpu.make_async_copy(
            (k_hbm, v_hbm)[kind].at[:, columns(head)],
            buffers[kind].at[me, head],
            load_sem.at[kind * kv_heads + head],
        )
        for kind, head in pieces
    ]
    load_order = pltpu.make_async_copy(order_hbm, order_ref, load_sem.at[2 * kv_heads])
    load_q = pltpu.make_async_copy(q_hbm, q_ref, load_sem.at[2 * kv_heads + 1])
    for load in loads:
        load.start()
    load_q.start()
    load_order.start()

    major = jnp.where(me < n // 2, -1, 1)

    def inside(index):
        return (index >= 0) & (index < n)

    barrier = pltpu.get_barrier_semaphore()
    for way in (-1, 1):
        @pl.when(inside(me + way))
        def _():
            pl.semaphore_signal(barrier, inc=1, device_id={"ctx": me + way}, device_id_type=MESH)

    pl.semaphore_wait(barrier, jnp.where(me > 0, 1, 0) + jnp.where(me < n - 1, 1, 0))

    def hop(way, kind, head, step, block):
        lane = (way + 1) // 2
        piece = kind * kv_heads + head
        return pltpu.make_async_remote_copy(
            src_ref=buffers[kind].at[block, head],
            dst_ref=buffers[kind].at[block, head],
            send_sem=send_sem.at[lane, piece, step],
            recv_sem=recv_sem.at[lane, piece, step],
            device_id={"ctx": jnp.clip(me + way, 0, n - 1)},
            device_id_type=MESH,
        )

    def arrive(kind, head, step):
        for way in (major, -major):
            @pl.when(inside(me - way * step))
            def _():
                hop(way, kind, head, step - 1, me - way * step).wait_recv()

                @pl.when(inside(me + way))
                def _():
                    hop(way, kind, head, step, me - way * step).start()

    for (kind, head), load in zip(pieces, loads):
        load.wait()
        for way in (major, -major):
            @pl.when(inside(me + way))
            def _():
                hop(way, kind, head, 0, me).start()

    load_q.wait()
    load_order.wait()

    def low_first(block):
        return order_ref[2 * block] < order_ref[2 * block + 1]

    def low_span(block):
        return jnp.minimum(order_ref[2 * block], order_ref[2 * block + 1])

    def low_high(ref, block, head):
        first, second = ref[block, head, :span], ref[block, head, span:]
        swap = low_first(block)
        return jnp.where(swap, first, second), jnp.where(swap, second, first)

    def score(head, part, keys):
        queries = stack_ref[head, part] if isinstance(part, int) else part
        return lax.dot_general(
            queries, keys, (((1,), (1,)), ((), ())), preferred_element_type=jnp.float32
        )

    def peak(scores):
        return jnp.max(scores, axis=1, keepdims=True)

    def weights_of(scores, top):
        return jnp.exp2((scores - top) * exponent_scale).astype(jnp.bfloat16)

    def keep(ref, value):
        ref[...] = jnp.broadcast_to(value, (group * span, HEAD_SIZE))

    def with_ones(values):
        return jnp.concatenate([values, jnp.ones_like(values)], axis=1)

    def product(weights, values):
        return jnp.dot(weights, with_ones(values), preferred_element_type=jnp.float32)

    mine_first = low_first(me)
    for head in range(kv_heads):
        for member in range(group):
            column = columns(head * group + member)
            first, second = q_ref[:span, column], q_ref[span:, column]
            stack_ref[head, 0, member * span : (member + 1) * span] = jnp.where(mine_first, first, second)
            stack_ref[head, 1, member * span : (member + 1) * span] = jnp.where(mine_first, second, first)

    tall = (group * span, span)
    row = lax.rem(lax.broadcasted_iota(jnp.int32, tall, 0), span)
    bias = jnp.where(lax.broadcasted_iota(jnp.int32, tall, 1) <= row, 0.0, MASKED)
    for head in range(kv_heads):
        key_low, key_high = low_high(k_ref, me, head)
        value_low, value_high = low_high(v_ref, me, head)
        low = score(head, 0, key_low) + bias
        low_top = peak(low)
        keep(top_ref.at[head, 0], low_top)
        acc_ref[head, 0] = product(weights_of(low, low_top), value_low)
        cross = score(head, 1, key_low)
        high = score(head, 1, key_high) + bias
        high_top = jnp.maximum(peak(cross), peak(high))
        keep(top_ref.at[head, 1], high_top)
        acc_ref[head, 1] = product(weights_of(cross, high_top), value_low) + product(
            weights_of(high, high_top), value_high
        )

    def weigh(block, head):
        earlier = low_span(block) < low_span(me)
        key_low, key_high = low_high(k_ref, block, head)
        cross = score(head, 1, key_low)
        other = score(
            head,
            jnp.where(earlier, stack_ref[head, 0], stack_ref[head, 1]),
            jnp.where(earlier, key_low, key_high),
        )
        other_top = peak(other)
        old_low, old_high = top_ref[head, 0][:, :1], top_ref[head, 1][:, :1]
        low_top = jnp.maximum(old_low, jnp.where(earlier, other_top, MASKED))
        high_top = jnp.maximum(
            jnp.maximum(old_high, peak(cross)), jnp.where(earlier, MASKED, other_top)
        )
        keep(top_ref.at[head, 0], low_top)
        keep(top_ref.at[head, 1], high_top)
        acc_ref[head, 0] *= jnp.exp2((old_low - low_top) * exponent_scale)
        acc_ref[head, 1] *= jnp.exp2((old_high - high_top) * exponent_scale)
        p_ref[head, 0] = weights_of(cross, high_top)
        p_ref[head, 1] = weights_of(other, jnp.where(earlier, low_top, high_top))

    def gather(block, head):
        earlier = low_span(block) < low_span(me)
        value_low, value_high = low_high(v_ref, block, head)
        cross = product(p_ref[head, 0], value_low)
        other = product(p_ref[head, 1], jnp.where(earlier, value_low, value_high))
        acc_ref[head, 0] += jnp.where(earlier, other, 0.0)
        acc_ref[head, 1] += cross + jnp.where(earlier, 0.0, other)

    def finish(head):
        for member in range(group):
            column = columns(head * group + member)
            part = pl.ds(member * span, span)
            low = acc_ref[head, 0, part, :HEAD_SIZE] / acc_ref[head, 0, part, HEAD_SIZE:]
            high = acc_ref[head, 1, part, :HEAD_SIZE] / acc_ref[head, 1, part, HEAD_SIZE:]
            out_ref[:span, column] = jnp.where(mine_first, low, high).astype(out_ref.dtype)
            out_ref[span:, column] = jnp.where(mine_first, high, low).astype(out_ref.dtype)

    def turn(step, last=False):
        for kind, work in ((KEY, weigh), (VALUE, gather)):
            for head in range(kv_heads):
                arrive(kind, head, step)

                @pl.when(inside(me - major * step))
                def _():
                    work(me - major * step, head)

                if last and kind == VALUE:
                    finish(head)

        if not last:
            @pl.when(inside(me + major * step))
            def _():
                for head in range(kv_heads):
                    weigh(me + major * step, head)
                    gather(me + major * step, head)

    lax.fori_loop(1, n - 1, lambda step, carry: turn(step) or carry, 0)
    turn(n - 1, last=True)

    def drain(step, carry):
        for kind, head in pieces:
            for way in (major, -major):
                @pl.when(inside(me - way * step) & inside(me + way))
                def _():
                    hop(way, kind, head, step, me - way * step).wait_send()
        return carry

    lax.fori_loop(0, n - 1, drain, 0)


def shards(n, queries, keys, values, span_order):
    rows, q_cols = queries.shape
    span = rows // 2
    kv_heads = keys.shape[1] // HEAD_SIZE
    tall = q_cols // HEAD_SIZE // kv_heads * span
    inputs = [pltpu.with_memory_space_constraint(x, pltpu.HBM) for x in (span_order, queries, keys, values)]
    return pl.pallas_call(
        functools.partial(attend, n),
        out_shape=jax.ShapeDtypeStruct((rows, q_cols), jnp.bfloat16),
        in_specs=[pl.BlockSpec(memory_space=pltpu.HBM)] * 4,
        out_specs=pl.BlockSpec(memory_space=pltpu.VMEM),
        scratch_shapes=[
            pltpu.SMEM(span_order.shape, jnp.int32),
            pltpu.VMEM((rows, q_cols), jnp.bfloat16),
            pltpu.VMEM((n, kv_heads, rows, HEAD_SIZE), jnp.bfloat16),
            pltpu.VMEM((n, kv_heads, rows, HEAD_SIZE), jnp.bfloat16),
            pltpu.VMEM((kv_heads, 2, tall, HEAD_SIZE), jnp.bfloat16),
            pltpu.VMEM((kv_heads, 2, tall, span), jnp.bfloat16),
            pltpu.VMEM((kv_heads, 2, tall, HEAD_SIZE), jnp.float32),
            pltpu.VMEM((kv_heads, 2, tall, 2 * HEAD_SIZE), jnp.float32),
            pltpu.SemaphoreType.DMA((2 * kv_heads + 2,)),
            pltpu.SemaphoreType.DMA((2, 2 * kv_heads, n)),
            pltpu.SemaphoreType.DMA((2, 2 * kv_heads, n)),
        ],
        compiler_params=pltpu.CompilerParams(
            collective_id=0, has_side_effects=True, vmem_limit_bytes=32 * 2**20
        ),
    )(*inputs)


def solution(mesh):
    split = P(("groups", "ctx"), ("head", "rep"))
    return jax.shard_map(
        functools.partial(shards, mesh.shape["ctx"]),
        mesh=mesh,
        in_specs=(split, split, split, P()),
        out_specs=split,
        check_vma=False,
    )
```

```python
import functools
import math

import jax
import jax.numpy as jnp
from jax import lax
from jax.experimental import pallas as pl
from jax.experimental.pallas import tpu as pltpu
from jax.sharding import PartitionSpec as P

HEAD_SIZE = 128
MASKED = -1e30
MESH = pl.DeviceIdType.MESH
KEY, VALUE = 0, 1


def attend(
    n, order_hbm, q_hbm, k_hbm, v_hbm, out_ref,
    order_ref, q_ref, k_ref, v_ref, stack_ref, p_ref, top_ref, total_ref, acc_ref,
    load_sem, send_sem, recv_sem,
):
    me = lax.axis_index("ctx")
    rows, q_cols = q_ref.shape
    span = rows // 2
    kv_heads = k_ref.shape[2] // HEAD_SIZE
    group = q_cols // HEAD_SIZE // kv_heads
    exponent_scale = math.log2(math.e) / math.sqrt(HEAD_SIZE)
    buffers = (k_ref, v_ref)

    load_k = pltpu.make_async_copy(k_hbm, k_ref.at[me], load_sem.at[0])
    load_v = pltpu.make_async_copy(v_hbm, v_ref.at[me], load_sem.at[1])
    load_order = pltpu.make_async_copy(order_hbm, order_ref, load_sem.at[3])
    load_q = pltpu.make_async_copy(q_hbm, q_ref, load_sem.at[2])
    load_k.start()
    load_v.start()
    load_q.start()
    load_order.start()

    major = jnp.where(me < n // 2, -1, 1)

    def inside(index):
        return (index >= 0) & (index < n)

    barrier = pltpu.get_barrier_semaphore()
    for way in (-1, 1):
        @pl.when(inside(me + way))
        def _():
            pl.semaphore_signal(barrier, inc=1, device_id={"ctx": me + way}, device_id_type=MESH)

    pl.semaphore_wait(barrier, jnp.where(me > 0, 1, 0) + jnp.where(me < n - 1, 1, 0))

    def hop(way, kind, step, block):
        lane = (way + 1) // 2
        return pltpu.make_async_remote_copy(
            src_ref=buffers[kind].at[block],
            dst_ref=buffers[kind].at[block],
            send_sem=send_sem.at[lane, kind, step],
            recv_sem=recv_sem.at[lane, kind, step],
            device_id={"ctx": jnp.clip(me + way, 0, n - 1)},
            device_id_type=MESH,
        )

    def arrive(kind, step):
        for way in (major, -major):
            @pl.when(inside(me - way * step))
            def _():
                hop(way, kind, step - 1, me - way * step).wait_recv()

                @pl.when(inside(me + way))
                def _():
                    hop(way, kind, step, me - way * step).start()

    for kind, load in ((KEY, load_k), (VALUE, load_v)):
        load.wait()
        for way in (major, -major):
            @pl.when(inside(me + way))
            def _():
                hop(way, kind, 0, me).start()

    load_q.wait()
    load_order.wait()

    def columns(head):
        return pl.ds(head * HEAD_SIZE, HEAD_SIZE)

    def low_first(block):
        return order_ref[2 * block] < order_ref[2 * block + 1]

    def low_span(block):
        return jnp.minimum(order_ref[2 * block], order_ref[2 * block + 1])

    def low_high(ref, block, head):
        first, second = ref[block, :span, columns(head)], ref[block, span:, columns(head)]
        swap = low_first(block)
        return jnp.where(swap, first, second), jnp.where(swap, second, first)

    def score(head, part, keys):
        queries = stack_ref[head, part] if isinstance(part, int) else part
        return lax.dot_general(
            queries, keys, (((1,), (1,)), ((), ())), preferred_element_type=jnp.float32
        )

    def peak(scores):
        return jnp.max(scores, axis=1, keepdims=True)

    def weights_of(scores, top):
        return jnp.exp2((scores - top) * exponent_scale).astype(jnp.bfloat16)

    def keep(ref, value):
        ref[...] = jnp.broadcast_to(value, (group * span, HEAD_SIZE))

    def product(weights, values):
        return jnp.dot(weights, values, preferred_element_type=jnp.float32)

    ones = jnp.ones((span, HEAD_SIZE), jnp.bfloat16)

    mine_first = low_first(me)
    for head in range(kv_heads):
        for member in range(group):
            column = columns(head * group + member)
            first, second = q_ref[:span, column], q_ref[span:, column]
            stack_ref[head, 0, member * span : (member + 1) * span] = jnp.where(mine_first, first, second)
            stack_ref[head, 1, member * span : (member + 1) * span] = jnp.where(mine_first, second, first)

    tall = (group * span, span)
    row = lax.rem(lax.broadcasted_iota(jnp.int32, tall, 0), span)
    bias = jnp.where(lax.broadcasted_iota(jnp.int32, tall, 1) <= row, 0.0, MASKED)
    for head in range(kv_heads):
        key_low, key_high = low_high(k_ref, me, head)
        value_low, value_high = low_high(v_ref, me, head)
        low = score(head, 0, key_low) + bias
        low_top = peak(low)
        keep(top_ref.at[head, 0], low_top)
        low_weights = weights_of(low, low_top)
        total_ref[head, 0] = product(low_weights, ones)
        acc_ref[head, 0] = product(low_weights, value_low)
        cross = score(head, 1, key_low)
        high = score(head, 1, key_high) + bias
        high_top = jnp.maximum(peak(cross), peak(high))
        keep(top_ref.at[head, 1], high_top)
        cross_weights, high_weights = weights_of(cross, high_top), weights_of(high, high_top)
        total_ref[head, 1] = product(cross_weights, ones) + product(high_weights, ones)
        acc_ref[head, 1] = product(cross_weights, value_low) + product(high_weights, value_high)

    def weigh(block):
        earlier = low_span(block) < low_span(me)
        for head in range(kv_heads):
            key_low, key_high = low_high(k_ref, block, head)
            cross = score(head, 1, key_low)
            other = score(
                head,
                jnp.where(earlier, stack_ref[head, 0], stack_ref[head, 1]),
                jnp.where(earlier, key_low, key_high),
            )
            other_top = peak(other)
            old_low, old_high = top_ref[head, 0][:, :1], top_ref[head, 1][:, :1]
            low_top = jnp.maximum(old_low, jnp.where(earlier, other_top, MASKED))
            high_top = jnp.maximum(
                jnp.maximum(old_high, peak(cross)), jnp.where(earlier, MASKED, other_top)
            )
            keep(top_ref.at[head, 0], low_top)
            keep(top_ref.at[head, 1], high_top)
            low_alpha = jnp.exp2((old_low - low_top) * exponent_scale)
            high_alpha = jnp.exp2((old_high - high_top) * exponent_scale)
            cross_weights = weights_of(cross, high_top)
            other_weights = weights_of(other, jnp.where(earlier, low_top, high_top))
            cross_total, other_total = product(cross_weights, ones), product(other_weights, ones)
            p_ref[head, 0] = cross_weights
            p_ref[head, 1] = other_weights
            acc_ref[head, 0] *= low_alpha
            acc_ref[head, 1] *= high_alpha
            total_ref[head, 0] = total_ref[head, 0] * low_alpha + jnp.where(earlier, other_total, 0.0)
            total_ref[head, 1] = (
                total_ref[head, 1] * high_alpha + cross_total + jnp.where(earlier, 0.0, other_total)
            )

    def gather(block):
        earlier = low_span(block) < low_span(me)
        for head in range(kv_heads):
            value_low, value_high = low_high(v_ref, block, head)
            cross = product(p_ref[head, 0], value_low)
            other = product(p_ref[head, 1], jnp.where(earlier, value_low, value_high))
            acc_ref[head, 0] += jnp.where(earlier, other, 0.0)
            acc_ref[head, 1] += cross + jnp.where(earlier, 0.0, other)

    def turn(step, last=False):
        arrive(KEY, step)

        @pl.when(inside(me - major * step))
        def _():
            weigh(me - major * step)

        if last:
            total_ref[...] = 1.0 / total_ref[...]
        arrive(VALUE, step)

        @pl.when(inside(me - major * step))
        def _():
            gather(me - major * step)

        if not last:
            @pl.when(inside(me + major * step))
            def _():
                weigh(me + major * step)
                gather(me + major * step)

    lax.fori_loop(1, n - 1, lambda step, carry: turn(step) or carry, 0)
    turn(n - 1, last=True)

    for head in range(kv_heads):
        for member in range(group):
            column = columns(head * group + member)
            part = pl.ds(member * span, span)
            low = acc_ref[head, 0, part] * total_ref[head, 0, part]
            high = acc_ref[head, 1, part] * total_ref[head, 1, part]
            out_ref[:span, column] = jnp.where(mine_first, low, high).astype(out_ref.dtype)
            out_ref[span:, column] = jnp.where(mine_first, high, low).astype(out_ref.dtype)

    def drain(step, carry):
        for kind in (KEY, VALUE):
            for way in (major, -major):
                @pl.when(inside(me - way * step) & inside(me + way))
                def _():
                    hop(way, kind, step, me - way * step).wait_send()
        return carry

    lax.fori_loop(0, n - 1, drain, 0)


def shards(n, queries, keys, values, span_order):
    rows, q_cols = queries.shape
    span = rows // 2
    kv_heads = keys.shape[1] // HEAD_SIZE
    tall = q_cols // HEAD_SIZE // kv_heads * span
    inputs = [pltpu.with_memory_space_constraint(x, pltpu.HBM) for x in (span_order, queries, keys, values)]
    return pl.pallas_call(
        functools.partial(attend, n),
        out_shape=jax.ShapeDtypeStruct((rows, q_cols), jnp.bfloat16),
        in_specs=[pl.BlockSpec(memory_space=pltpu.HBM)] * 4,
        out_specs=pl.BlockSpec(memory_space=pltpu.VMEM),
        scratch_shapes=[
            pltpu.SMEM(span_order.shape, jnp.int32),
            pltpu.VMEM((rows, q_cols), jnp.bfloat16),
            pltpu.VMEM((n,) + keys.shape, jnp.bfloat16),
            pltpu.VMEM((n,) + values.shape, jnp.bfloat16),
            pltpu.VMEM((kv_heads, 2, tall, HEAD_SIZE), jnp.bfloat16),
            pltpu.VMEM((kv_heads, 2, tall, span), jnp.bfloat16),
            pltpu.VMEM((kv_heads, 2, tall, HEAD_SIZE), jnp.float32),
            pltpu.VMEM((kv_heads, 2, tall, HEAD_SIZE), jnp.float32),
            pltpu.VMEM((kv_heads, 2, tall, HEAD_SIZE), jnp.float32),
            pltpu.SemaphoreType.DMA((4,)),
            pltpu.SemaphoreType.DMA((2, 2, n)),
            pltpu.SemaphoreType.DMA((2, 2, n)),
        ],
        compiler_params=pltpu.CompilerParams(
            collective_id=0, has_side_effects=True, vmem_limit_bytes=32 * 2**20
        ),
    )(*inputs)


def solution(mesh):
    split = P(("groups", "ctx"), ("head", "rep"))
    return jax.shard_map(
        functools.partial(shards, mesh.shape["ctx"]),
        mesh=mesh,
        in_specs=(split, split, split, P()),
        out_specs=split,
        check_vma=False,
    )
```
